32 devices in a mesh: expert: 8 (over z, y), vocab: 4 (over x, core).
Axes of the slice: x: 2, y: 2, z: 4, core: 2. Of those that a mesh axis runs over, the one named last changes fastest.
Arguments:
- tokens: bfloat16 [2048, 2048], P('expert'), may hold values from -6 to 6
- teacher_expert: int32 [2048, 1], P('expert'), may hold values from 0 to 3
- student_expert: int32 [2048, 1], P('expert'), may hold values from 0 to 3
- priority: int32 [8, 256], P('expert'), may hold values from 0 to 255, each once within a row
- expert_in: bfloat16 [8, 2048, 8192], P('expert', None, 'vocab'), may hold values from -0.125 to 0.125
- expert_out: bfloat16 [8, 8192, 2048], P('expert', 'vocab'), may hold values from -0.0625 to 0.0625
- teacher_gain: float32 [2048], replicated, may hold values from 0.1 to 1.9
- student_gain: float32 [2048], replicated, may hold values from 0.1 to 1.9
- teacher_head: bfloat16 [8192, 2048], P(('vocab', 'expert')), may hold values from -4 to 4
- student_head: bfloat16 [8192, 2048], P(('vocab', 'expert')), may hold values from -4 to 4
Outputs:
- token_kl: float32 [2048], P('expert')
The draws below stay inside these ranges and needn't reach their ends.
Inputs may be any that keep to these rules, and one draw needn't show every extreme that they name: Each row of priority holds every number of 0 to 255 once.
All inputs are finite; a program needn't handle non-finite values.
Results may differ from the reference program's by a relative error of at most 0.0032.
Values may be sent and summed in bfloat16 or wider, within the bound.
No kernel may reach another device: no remote copies, remote signals or barrier semaphores. Data moves between devices by JAX's collectives and lax.ppermute only.
A program may use at most 128 MiB of HBM per device.

```python
import math
import jax
import jax.numpy as jnp
from jax import lax

D = 2048
FF = 8192
TOK_DEV = 256
CAP = 96
TOKENS = 2048
VOCAB = 8192
N_EXPERT = 8


def head_matrix(key):
    normal_key, spread_key = jax.random.split(key, 2)
    entries = jax.random.normal(normal_key, (VOCAB, D), jnp.float32)
    vocab_ramp = 1.0 + 2.0 * jnp.arange(VOCAB, dtype=jnp.float32) / VOCAB
    spread = jnp.exp(jax.random.uniform(spread_key, (VOCAB, 1), jnp.float32, math.log(0.3), math.log(3.0)))
    row_scale = spread * vocab_ramp[:, None] / math.sqrt(D)
    matrix = entries * row_scale
    return jnp.clip(matrix, -4.0, 4.0)


def draw_teacher_head(key, part):
    return head_matrix(jax.random.fold_in(key, 101)).astype(jnp.bfloat16)


def draw_student_head(key, part):
    return head_matrix(jax.random.fold_in(key, 202)).astype(jnp.bfloat16)


def steps_of(key, extent, shards, least, top_value):
    def one(dim, blocks):
        steps = jax.random.uniform(jax.random.fold_in(jax.random.fold_in(key, 6), dim), (blocks,), jnp.float32, least / len(shards), top_value / len(shards))
        return jnp.repeat(jnp.exp(steps), extent[dim] // blocks).reshape((-1,) + (1,) * (len(extent) - dim - 1))

    level = one(*shards[0])
    for cut in shards[1:]:
        level = level * one(*cut)
    return level


def picks_of(own_key, rows, number_of, top, lift):
    order = jax.random.permutation(jax.random.fold_in(own_key, 1), number_of)
    pull = order
    for power in range(3):
        pull = pull * pull // number_of
    pull = pull * lift // number_of
    lots = jax.random.randint(jax.random.fold_in(own_key, 2), (rows, number_of), 0, 4096) + pull
    sure = jax.random.permutation(jax.random.fold_in(own_key, 3), rows)[jnp.arange(number_of) % rows]
    lots = jnp.where(jnp.arange(rows)[:, None] == sure[None, :], 1 << 14, lots)
    merit = lots * number_of + jnp.arange(number_of)
    return lax.top_k(merit.astype(jnp.int32), top)[1].astype(jnp.int32)


def gaussian(rng, extent, scale, most, cuts=(), held_as=jnp.bfloat16):
    factor_of = steps_of(rng, extent, cuts, -0.22, 0.18) if cuts else 1.0
    array = jax.random.normal(rng, extent, jnp.float32) * scale * factor_of
    return jnp.minimum(jnp.maximum(array, -most), most).astype(held_as)


def setup_inputs(seed: int = 0) -> dict:
    key_of = jax.random.split(jax.random.key(seed), 11)
    tokens = gaussian(key_of[0], (TOKENS, D), 1.0, 6.0, ((0, 8),))
    teacher_expert = picks_of(key_of[1], TOKENS, N_EXPERT // 2, 1, 2048)
    student_expert = picks_of(key_of[2], TOKENS, N_EXPERT // 2, 1, 2048)
    priority = jax.vmap(lambda own: jax.random.permutation(own, TOK_DEV))(jax.random.split(key_of[3], N_EXPERT)).reshape((N_EXPERT, TOK_DEV)).astype(jnp.int32)
    expert_in = gaussian(key_of[4], (N_EXPERT, D, FF), D ** -0.5, 0.125, ((0, 8), (2, 4)))
    expert_out = gaussian(key_of[5], (N_EXPERT, FF, D), FF ** -0.5, 0.0625, ((0, 8), (1, 4)))
    teacher_gain = jnp.clip(1.0 + 0.18 * jax.random.normal(key_of[6], (D,), jnp.float32), 0.1, 1.9)
    student_gain = jnp.clip(1.0 + 0.18 * jax.random.normal(key_of[7], (D,), jnp.float32), 0.1, 1.9)
    teacher_head = draw_teacher_head(jax.random.fold_in(key_of[10], 71), 0)
    student_head = draw_student_head(jax.random.fold_in(key_of[10], 71), 0)
    return {"tokens": tokens, "teacher_expert": teacher_expert, "student_expert": student_expert, "priority": priority, "expert_in": expert_in, "expert_out": expert_out, "teacher_gain": teacher_gain, "student_gain": student_gain, "teacher_head": teacher_head, "student_head": student_head}


def slot_places(expert, ranking, capacity, lane, dump):
    same_expert = expert[:, None] == expert[None, :]
    before = ranking[None, :] < ranking[:, None]
    slot_rank = lax.optimization_barrier(jnp.sum(jnp.logical_and(same_expert, before).astype(jnp.int32), axis=1))
    kept_mask = slot_rank < capacity
    return jnp.where(kept_mask, (2 * expert + lane) * capacity + slot_rank, dump).astype(jnp.int32)

def normed(tokens, branch, gain_vector):
    summed = tokens.astype(jnp.float32) + branch.astype(jnp.float32)
    factor = lax.rsqrt(lax.optimization_barrier(jnp.mean(summed * summed, axis=-1, keepdims=True)) + 1e-05)
    return (summed * factor * gain_vector).astype(jnp.bfloat16)

def reference(tokens, teacher_expert, student_expert, priority, expert_in, expert_out, teacher_gain, student_gain, teacher_head, student_head):
    groups = N_EXPERT
    dump = groups * CAP
    blocks = tokens.reshape(groups, TOK_DEV, D)
    teacher_ids = teacher_expert.reshape(groups, TOK_DEV)
    student_ids = student_expert.reshape(groups, TOK_DEV)
    teacher_places = jax.vmap(slot_places, in_axes=(0, 0, None, None, None))(teacher_ids, priority, CAP, 0, dump)
    student_places = jax.vmap(slot_places, in_axes=(0, 0, None, None, None))(student_ids, priority, CAP, 1, dump)
    numbers = jnp.arange(TOK_DEV, dtype=jnp.int32)

    def owners_of(first, second):
        filled = jnp.full((dump + 1,), TOK_DEV, jnp.int32).at[first].set(numbers).at[second].set(numbers)
        return filled[:dump]
    owners = jax.vmap(owners_of)(teacher_places, student_places)
    padded = jnp.concatenate([blocks, jnp.zeros((groups, 1, D), jnp.bfloat16)], axis=1)
    outgoing = jax.vmap(lambda source, picked: source[picked])(padded, owners).reshape(groups, groups, CAP, D)

    def run_expert(index):
        received = outgoing[:, index].reshape(groups * CAP, D)
        hidden = jax.nn.gelu(jnp.dot(received, expert_in[index], preferred_element_type=jnp.float32)).astype(jnp.bfloat16)
        result = jnp.dot(hidden, expert_out[index], preferred_element_type=jnp.float32).astype(jnp.bfloat16)
        return result.reshape(groups, CAP, D)
    results = lax.map(run_expert, jnp.arange(groups, dtype=jnp.int32))
    returned = jnp.transpose(results, (1, 0, 2, 3)).reshape(groups, dump, D)
    returned = jnp.concatenate([returned, jnp.zeros((groups, 1, D), jnp.bfloat16)], axis=1)
    teacher_branch = jax.vmap(lambda source, picked: source[picked])(returned, teacher_places)
    student_branch = jax.vmap(lambda source, picked: source[picked])(returned, student_places)
    teacher_normed = normed(blocks, teacher_branch, teacher_gain)
    student_normed = normed(blocks, student_branch, student_gain)

    def block_loss(paired):
        teacher_rows, student_rows = paired
        teacher_logits = jnp.dot(teacher_rows, teacher_head.T, preferred_element_type=jnp.float32)
        student_logits = jnp.dot(student_rows, student_head.T, preferred_element_type=jnp.float32)
        teacher_log = jax.nn.log_softmax(teacher_logits, axis=-1)
        student_log = jax.nn.log_softmax(student_logits, axis=-1)
        return lax.optimization_barrier(jnp.sum(jnp.exp(teacher_log) * (teacher_log - student_log), axis=-1))
    return lax.map(block_loss, (teacher_normed, student_normed)).reshape(TOKENS)
```

```python
import jax
import jax.numpy as jnp
from jax import lax
from jax.sharding import PartitionSpec as P


BOTH = ("expert", "vocab")


def slot_ranks(expert, ranking):
    same_expert = expert[:, None] == expert[None, :]
    before = ranking[None, :] < ranking[:, None]
    return jnp.sum(jnp.logical_and(same_expert, before).astype(jnp.int32), axis=1)


def ffn(rows, weight_in, weight_out):
    hidden = jax.nn.gelu(
        jnp.dot(rows, weight_in, preferred_element_type=jnp.float32)
    ).astype(jnp.bfloat16)
    return jnp.dot(hidden, weight_out, preferred_element_type=jnp.float32).astype(jnp.bfloat16)


def set_of(w):
    return (w & 1) | ((w >> 2) << 1), (w >> 1) & 1


def block_of(x, zl):
    return (x & 1) | (zl << 1) | ((x >> 1) << 2)


def local(
    tokens,
    teacher_expert,
    student_expert,
    priority,
    expert_in,
    expert_out,
    teacher_gain,
    student_gain,
    teacher_head,
    student_head,
):
    count, width = tokens.shape
    En = lax.axis_size("expert")
    Vn = lax.axis_size("vocab")
    J = En // Vn
    H = En // 4
    X = Vn // 2
    cap = 3 * count // En
    hc = cap // 2
    hcnt = count // 2
    e = lax.axis_index("expert")
    v = lax.axis_index("vocab")
    x, c = v // 2, v % 2
    zh, zl, y = e // 4, (e // 2) % 2, e % 2

    def by_expert(array, move):
        return lax.ppermute(array, "expert", [(s, move(s)) for s in range(En)])

    def by_vocab(array, move):
        return lax.ppermute(array, "vocab", [(s, move(s)) for s in range(Vn)])

    def by_both(array, move):
        perm = []
        for s in range(En):
            for u in range(Vn):
                de, dv = move(s, u)
                perm.append((s * Vn + u, de * Vn + dv))
        return lax.ppermute(array, BOTH, perm)

    other_core = lambda array: by_vocab(array, lambda u: u ^ 1)

    ranking = priority[0]
    codes = []
    for expert in (teacher_expert[:, 0], student_expert[:, 0]):
        rank = slot_ranks(expert, ranking)
        codes.append(jnp.where(rank < cap, expert * cap + rank, -1))

    group_rows = jnp.arange(En * hc, dtype=jnp.int32)[:, None]
    chosen = jnp.zeros((En * hc, count), jnp.bool_)
    for lane, code in enumerate(codes):
        slot = code % cap
        target = (2 * (code // cap) + lane) ^ e
        mine = jnp.logical_and(code >= 0, slot // hc == c)
        place = jnp.where(mine, target * hc + slot % hc, -1)
        chosen = jnp.logical_or(chosen, group_rows == place[None, :])
    outgoing = jnp.dot(chosen.astype(jnp.bfloat16), tokens, preferred_element_type=jnp.float32)
    outgoing = outgoing.astype(jnp.bfloat16).reshape(En, hc, width)

    order = [m1 * 2 + (xi & 1) + ((xi >> 1) << 2) for m1 in range(2) for xi in range(X)]
    arrived = {}
    for r in range(J):
        for m in range(Vn):
            g = r * Vn + m
            arrived[g] = outgoing[g] if g == 0 else by_expert(outgoing[g], lambda s: s ^ g)

    def set_route(rho):
        def move(s, u):
            i = (s // Vn) ^ rho
            q = i * Vn + u
            xd, zld = set_of(s % Vn)
            return (q >> 2) * 4 + zld * 2 + ((q >> 1) & 1), 2 * xd + (q & 1)

        return move

    half_tokens = lax.dynamic_slice_in_dim(tokens, c * hcnt, hcnt, 0)
    half_codes = lax.dynamic_slice_in_dim(jnp.stack(codes), c * hcnt, hcnt, 1)

    def over_x(shards):
        stacked = jnp.stack(shards)
        return [by_vocab(stacked, lambda u: u ^ (2 * d)) for d in range(1, X)]

    def over_zl(shards):
        return by_expert(jnp.stack(shards), lambda s: s ^ 2)

    first = [arrived[g] for g in range(Vn)]
    first, heads = lax.optimization_barrier((first, (teacher_head, student_head)))
    for g in range(Vn):
        arrived[g] = first[g]
    t_head, s_head = heads
    t_row = [t_head] + [a[0] for a in over_x([t_head])]
    t_far = over_zl(t_row)
    t_heads = jnp.concatenate([jnp.stack(t_row), t_far]).reshape(-1, width)
    s_pair = jnp.concatenate([s_head[None], over_zl([s_head])])
    s_all = [s_pair] + over_x([s_pair[0], s_pair[1]])
    s_heads = jnp.stack(s_all, axis=1).reshape(-1, width)

    weight_in = expert_in[0]
    weight_out = expert_out[0]
    xe, _ = set_of(e % Vn)
    landed = []
    for r in range(J):
        own = jnp.stack([arrived[r * Vn + m] for m in order]).reshape(Vn * hc, width)
        rows = jnp.concatenate([own, other_core(own)], axis=0)
        partial = ffn(rows, weight_in, weight_out).reshape(2, 2, X, hc, width)
        kept_side = zl ^ c
        sent = lax.dynamic_index_in_dim(partial, 1 - kept_side, 1, keepdims=False)
        kept = lax.dynamic_index_in_dim(partial, kept_side, 1, keepdims=False)
        got = other_core(sent)
        summed = kept.astype(jnp.float32) + got[::-1].astype(jnp.float32)
        total = lax.dynamic_index_in_dim(summed, xe ^ x, 1, keepdims=False)
        narrow = summed.astype(jnp.bfloat16)
        for d in range(1, X):
            part = lax.dynamic_index_in_dim(narrow, xe ^ x ^ d, 1, keepdims=False)
            total = total + by_vocab(part, lambda u: u ^ (2 * d)).astype(jnp.float32)
        reduced = total.astype(jnp.bfloat16).reshape(cap, width)
        for q in range(H):

            def spread(s, u):
                return ((s // 4) ^ q) * 4 + (u % 2) * 2 + s % 2, (u // 2) * 2 + (s // 2) % 2

            landed.append(by_both(reduced, spread))

    set_tokens = jnp.concatenate([by_both(half_tokens, set_route(rho)) for rho in range(J)])
    set_codes = jnp.concatenate([by_both(half_codes, set_route(rho)) for rho in range(J)], axis=1)

    landed = jnp.stack(landed).reshape(J * H * cap, width)
    pool = jnp.concatenate([landed, other_core(landed)], axis=0)
    code = jnp.where(y == 0, set_codes[0], set_codes[1])
    me = ((zh * 2 + y) * 2 + c) // Vn
    block_j = me ^ (jnp.arange(J * hcnt, dtype=jnp.int32) // hcnt)
    source = 2 * (code // cap) + y
    slot = code % cap
    place = (source // 2 % 2) ^ c
    place = place * J + (block_j ^ (source // Vn))
    place = place * H + ((source // 4) ^ zh)
    place = place * cap + ((slot // hc) ^ zl) * hc + slot % hc
    place = jnp.where(code >= 0, place, -1)
    picked = place[:, None] == jnp.arange(2 * J * H * cap, dtype=jnp.int32)[None, :]
    branch = jnp.dot(picked.astype(jnp.bfloat16), pool, preferred_element_type=jnp.float32)
    gain = jnp.where(y == 0, teacher_gain, student_gain)
    total = set_tokens.astype(jnp.float32) + branch
    factor = lax.rsqrt(jnp.mean(total * total, axis=-1, keepdims=True) + 1e-05)
    own_normed = (total * factor * gain).astype(jnp.bfloat16)
    far_normed = by_expert(own_normed, lambda s: s ^ 1)
    teacher_half = jnp.where(y == 0, own_normed, far_normed)
    student_half = jnp.where(y == 0, far_normed, own_normed)
    teacher_normed = jnp.concatenate([teacher_half, other_core(teacher_half)])
    student_normed = jnp.concatenate([student_half, other_core(student_half)])

    contract = (((1,), (1,)), ((), ()))
    teacher_logits = lax.dot_general(
        teacher_normed, t_heads, contract, preferred_element_type=jnp.float32
    )
    student_logits = lax.dot_general(
        student_normed, s_heads, contract, preferred_element_type=jnp.float32
    )
    teacher_peak = jnp.max(teacher_logits, axis=1)
    student_peak = jnp.max(student_logits, axis=1)
    teacher_exps = jnp.exp(teacher_logits - teacher_peak[:, None])
    teacher_total = jnp.sum(teacher_exps, axis=1)
    weighted = jnp.sum(teacher_exps * (teacher_logits - student_logits), axis=1)
    student_total = jnp.sum(jnp.exp(student_logits - student_peak[:, None]), axis=1)

    def merge(parts, axis):
        tp, tt, tw, sp, st = [jnp.take(parts, i, axis=axis + 1) for i in range(5)]
        tpm = jnp.max(tp, axis=axis, keepdims=True)
        spm = jnp.max(sp, axis=axis, keepdims=True)
        tr = jnp.exp(tp - tpm)
        sr = jnp.exp(sp - spm)
        return (
            jnp.squeeze(tpm, axis),
            jnp.sum(tt * tr, axis=axis),
            jnp.sum(tw * tr, axis=axis),
            jnp.squeeze(spm, axis),
            jnp.sum(st * sr, axis=axis),
        )

    stats = jnp.stack([teacher_peak, teacher_total, weighted, student_peak, student_total])
    stats = stats.reshape(5, 2, J, hcnt)
    everyone = lax.all_gather(stats, "vocab", axis=0).reshape(X, 2, 5, 2, J, hcnt)
    aligned = jnp.stack([everyone[:, 0], everyone[:, 1, :, ::-1]], axis=1)
    by_x = jnp.stack(merge(aligned, 1), axis=1)
    by_x = jnp.take(by_x, me ^ jnp.arange(J), axis=3)
    neutral = jnp.array([-1e30, 0.0, 0.0, -1e30, 0.0], jnp.float32)[:, None, None]
    letters = []
    for b in range(En):
        xb, zb = set_of(b % Vn)
        letters.append(jnp.where(zl == zb, by_x[xb, :, :, b // Vn], neutral))
    mail = lax.all_to_all(jnp.stack(letters), "expert", split_axis=0, concat_axis=0, tiled=True)
    tp, tt, tw, sp, st = merge(mail, 0)
    kl = tw / tt - tp - jnp.log(tt) + sp + jnp.log(st)
    return kl.reshape(count)


def solution(mesh):
    in_specs = (
        P("expert", None),
        P("expert", None),
        P("expert", None),
        P("expert", None),
        P("expert", None, "vocab"),
        P("expert", "vocab", None),
        P(),
        P(),
        P(("vocab", "expert"), None),
        P(("vocab", "expert"), None),
    )
    out_specs = P("expert")
    return jax.shard_map(local, mesh=mesh, in_specs=in_specs, out_specs=out_specs, check_vma=False)
```

```python
import jax
import jax.numpy as jnp
from jax import lax
from jax.experimental import pallas as pl
from jax.experimental.pallas import tpu as pltpu
from jax.sharding import PartitionSpec as P


BOTH = ("expert", "vocab")


def slot_ranks(expert, ranking):
    same_expert = expert[:, None] == expert[None, :]
    before = ranking[None, :] < ranking[:, None]
    return jnp.sum(jnp.logical_and(same_expert, before).astype(jnp.int32), axis=1)


def ffn(rows, weight_in, weight_out):
    hidden = jax.nn.gelu(
        jnp.dot(rows, weight_in, preferred_element_type=jnp.float32)
    ).astype(jnp.bfloat16)
    return jnp.dot(hidden, weight_out, preferred_element_type=jnp.float32).astype(jnp.bfloat16)


def set_of(w):
    return (w & 1) | ((w >> 2) << 1), (w >> 1) & 1


def finish(flip, places, gains, tokens, pools, t_shards, s_shards):
    width = gains.shape[-1]
    piece = tokens[0].shape[0]
    rows = piece * len(tokens)
    tile = min(rows, 256)
    height = pools[0].shape[1]
    reach = height * len(pools)
    entries = t_shards[0].shape[0]
    span = entries * len(t_shards)
    shards = list(t_shards) + list(s_shards)
    counts = (len(tokens), len(pools), len(shards))

    def kernel(flip_ref, place_ref, gain_ref, *refs):
        token_in, refs = refs[: counts[0]], refs[counts[0] :]
        pool_in, refs = refs[: counts[1]], refs[counts[1] :]
        head_in, refs = refs[: counts[2]], refs[counts[2] :]
        out_ref, token, pool, head, normed, logits, token_sem, pool_sem, head_sem = refs
        copies = {}
        for branch in range(2):
            for i in range(counts[1]):
                copies["pool", branch, i] = pltpu.make_async_copy(
                    pool_in[i].at[flip_ref[0] ^ branch],
                    pool.at[branch, pl.ds(i * height, height)],
                    pool_sem.at[branch, i],
                )
                copies["pool", branch, i].start()
            if branch == 0:
                for i in range(counts[0]):
                    copies["token", i] = pltpu.make_async_copy(
                        token_in[i], token.at[pl.ds(i * piece, piece)], token_sem.at[i]
                    )
                    copies["token", i].start()
        for i in range(counts[2]):
            copies["head", i] = pltpu.make_async_copy(head_in[i], head.at[i], head_sem.at[i])
            copies["head", i].start()
        for branch in range(2):
            for i in range(counts[1]):
                copies["pool", branch, i].wait()
            if branch == 0:
                for i in range(counts[0]):
                    copies["token", i].wait()
            for t in range(rows // tile):
                here = pl.ds(t * tile, tile)
                number = lax.broadcasted_iota(jnp.int32, (tile, reach), 1)
                picked = jnp.where(number == place_ref[branch, here], 1.0, 0.0)
                total = token[here, :].astype(jnp.float32) + jnp.dot(
                    picked.astype(jnp.bfloat16), pool[branch], preferred_element_type=jnp.float32
                )
                mean = jnp.mean(total * total, axis=-1, keepdims=True)
                scaled = total * lax.rsqrt(mean + 1e-05) * gain_ref[branch]
                normed[branch, here, :] = scaled.astype(jnp.bfloat16)
        for i in range(counts[2]):
            copies["head", i].wait()
            branch, part = divmod(i, len(t_shards))
            logits[branch, :, part * entries : (part + 1) * entries] = lax.dot_general(
                normed[branch],
                head[i],
                (((1,), (1,)), ((), ())),
                preferred_element_type=jnp.float32,
            )
        for t in range(rows // tile):
            here = pl.ds(t * tile, tile)
            teacher, student = logits[0, here, :], logits[1, here, :]
            tp = jnp.max(teacher, axis=1, keepdims=True)
            sp = jnp.max(student, axis=1, keepdims=True)
            te = jnp.exp(teacher - tp)
            columns = [
                tp,
                jnp.sum(te, axis=1, keepdims=True),
                jnp.sum(te * (teacher - student), axis=1, keepdims=True),
                sp,
                jnp.sum(jnp.exp(student - sp), axis=1, keepdims=True),
            ]
            lane = lax.broadcasted_iota(jnp.int32, (tile, 128), 1)
            table = jnp.zeros((tile, 128), jnp.float32)
            for i, column in enumerate(columns):
                table = jnp.where(lane == i, column, table)
            out_ref[:, t * tile : (t + 1) * tile] = table.T[:8]

    return pl.pallas_call(
        kernel,
        in_specs=[
            pl.BlockSpec(memory_space=pltpu.SMEM),
            pl.BlockSpec(memory_space=pltpu.VMEM),
            pl.BlockSpec(memory_space=pltpu.VMEM),
        ]
        + [pl.BlockSpec(memory_space=pl.ANY)] * sum(counts),
        out_specs=pl.BlockSpec(memory_space=pltpu.VMEM),
        out_shape=jax.ShapeDtypeStruct((8, rows), jnp.float32),
        scratch_shapes=[
            pltpu.VMEM((rows, width), jnp.bfloat16),
            pltpu.VMEM((2, reach, width), jnp.bfloat16),
            pltpu.VMEM((len(shards), entries, width), jnp.bfloat16),
            pltpu.VMEM((2, rows, width), jnp.bfloat16),
            pltpu.VMEM((2, rows, span), jnp.float32),
            pltpu.SemaphoreType.DMA((counts[0],)),
            pltpu.SemaphoreType.DMA((2, counts[1])),
            pltpu.SemaphoreType.DMA((counts[2],)),
        ],
        name="finish",
    )(flip, places, gains, *tokens, *pools, *shards)


def local(
    tokens,
    teacher_expert,
    student_expert,
    priority,
    expert_in,
    expert_out,
    teacher_gain,
    student_gain,
    teacher_head,
    student_head,
):
    count, width = tokens.shape
    En = lax.axis_size("expert")
    Vn = lax.axis_size("vocab")
    J = En // Vn
    H = En // 4
    X = Vn // 2
    cap = 3 * count // En
    hc = cap // 2
    hcnt = count // 2
    e = lax.axis_index("expert")
    v = lax.axis_index("vocab")
    x, c = v // 2, v % 2
    zh, zl, y = e // 4, (e // 2) % 2, e % 2

    def by_expert(array, move):
        return lax.ppermute(array, "expert", [(s, move(s)) for s in range(En)])

    def by_vocab(array, move):
        return lax.ppermute(array, "vocab", [(s, move(s)) for s in range(Vn)])

    def by_both(array, move):
        perm = []
        for s in range(En):
            for u in range(Vn):
                de, dv = move(s, u)
                perm.append((s * Vn + u, de * Vn + dv))
        return lax.ppermute(array, BOTH, perm)

    other_core = lambda array: by_vocab(array, lambda u: u ^ 1)

    ranking = priority[0]
    codes = []
    for expert in (teacher_expert[:, 0], student_expert[:, 0]):
        rank = slot_ranks(expert, ranking)
        codes.append(jnp.where(rank < cap, expert * cap + rank, -1))

    group_rows = jnp.arange(En * hc, dtype=jnp.int32)[:, None]
    chosen = jnp.zeros((En * hc, count), jnp.bool_)
    for lane, code in enumerate(codes):
        slot = code % cap
        target = (2 * (code // cap) + lane) ^ e
        mine = jnp.logical_and(code >= 0, slot // hc == c)
        place = jnp.where(mine, target * hc + slot % hc, -1)
        chosen = jnp.logical_or(chosen, group_rows == place[None, :])
    outgoing = jnp.dot(chosen.astype(jnp.bfloat16), tokens, preferred_element_type=jnp.float32)
    outgoing = outgoing.astype(jnp.bfloat16).reshape(En, hc, width)

    order = [m1 * 2 + (xi & 1) + ((xi >> 1) << 2) for m1 in range(2) for xi in range(X)]
    arrived = {0: outgoing[0]}
    for g in range(1, En):
        arrived[g] = by_expert(outgoing[g], lambda s: s ^ g)

    t_shards, s_shards = [teacher_head], [student_head]
    for d in range(1, X):
        t_shards.append(by_vocab(teacher_head, lambda u: u ^ (2 * d)))
        s_shards.append(by_vocab(student_head, lambda u: u ^ (2 * d)))
    s_far = by_expert(student_head, lambda s: s ^ 2)
    t_far = by_expert(teacher_head, lambda s: s ^ 2)
    t_diag = [by_expert(t_shards[d], lambda s: s ^ 2) for d in range(1, X)]
    s_diag = [by_vocab(s_far, lambda u: u ^ (2 * d)) for d in range(1, X)]
    t_shards += [t_far] + t_diag
    s_shards += [s_far] + s_diag

    def set_route(rho):
        def move(s, u):
            i = (s // Vn) ^ rho
            q = i * Vn + u
            xd, zld = set_of(s % Vn)
            return (q >> 2) * 4 + zld * 2 + ((q >> 1) & 1), 2 * xd + (q & 1)

        return move

    half_tokens = lax.dynamic_slice_in_dim(tokens, c * hcnt, hcnt, 0)
    numbers = [f(code) for code in codes for f in (lambda a: a // cap, lambda a: a % cap)]
    numbers = jnp.concatenate(numbers).astype(jnp.bfloat16)
    tail = -(-numbers.size // (16 * width)) * 16
    numbers = jnp.pad(numbers, (0, tail * width - numbers.size)).reshape(tail, width)
    parcel = jnp.concatenate([half_tokens, numbers])
    parcels = [by_both(parcel, set_route(rho)) for rho in range(J)]
    set_tokens = [parcel[:hcnt] for parcel in parcels]
    set_tokens += [other_core(array) for array in set_tokens]
    numbers = [parcel[hcnt:].reshape(-1)[: 4 * count] for parcel in parcels]
    numbers = jnp.stack(numbers).astype(jnp.int32).reshape(J, 2, 2, 2, hcnt)
    numbers = jnp.where(c == 0, numbers, numbers[:, :, :, ::-1])
    set_codes = jnp.transpose(numbers, (1, 2, 3, 0, 4)).reshape(2, 2, 2 * J * hcnt)

    weight_in = expert_in[0]
    weight_out = expert_out[0]
    xe, _ = set_of(e % Vn)
    pools = []
    for r in range(J):
        own = jnp.stack([arrived[r * Vn + m] for m in order]).reshape(Vn * hc, width)
        rows = jnp.concatenate([own, other_core(own)], axis=0)
        partial = ffn(rows, weight_in, weight_out).reshape(2, 2, X, hc, width)
        kept_side = zl ^ c
        sent = lax.dynamic_index_in_dim(partial, 1 - kept_side, 1, keepdims=False)
        kept = lax.dynamic_index_in_dim(partial, kept_side, 1, keepdims=False)
        got = other_core(sent)
        summed = kept.astype(jnp.float32) + got[::-1].astype(jnp.float32)
        total = lax.dynamic_index_in_dim(summed, xe ^ x, 1, keepdims=False)
        narrow = summed.astype(jnp.bfloat16)
        for d in range(1, X):
            part = lax.dynamic_index_in_dim(narrow, xe ^ x ^ d, 1, keepdims=False)
            part = by_vocab(part, lambda u: u ^ (2 * d))
            total = total + part.astype(jnp.float32)
        reduced = total.astype(jnp.bfloat16).reshape(cap, width)
        mine, crossed = [], []
        for q in range(H):

            def spread(s, u):
                return ((s // 4) ^ q) * 4 + (u % 2) * 2 + s % 2, (u // 2) * 2 + (s // 2) % 2

            mine.append(by_both(reduced, spread))
            crossed.append(by_expert(mine[-1], lambda s: s ^ 1))
        mine = jnp.stack(mine + crossed).reshape(2, H * cap, width)
        pools += [mine, other_core(mine)]

    me = ((zh * 2 + y) * 2 + c) // Vn
    block_j = me ^ (jnp.arange(2 * J * hcnt, dtype=jnp.int32) // hcnt % J)
    places = []
    for lane in range(2):
        chosen_expert, slot = set_codes[lane]
        source = 2 * chosen_expert + lane
        place = (block_j ^ (source // Vn)) * 2 + ((source // 2 % 2) ^ c)
        place = place * H + ((source // 4) ^ zh)
        place = place * cap + ((slot // hc) ^ zl) * hc + slot % hc
        places.append(jnp.where(chosen_expert >= 0, place, -1))
    stats = finish(
        jnp.reshape(y, (1,)).astype(jnp.int32),
        jnp.stack(places)[:, :, None],
        jnp.stack([teacher_gain, student_gain])[:, None, :],
        set_tokens,
        pools,
        t_shards,
        s_shards,
    )

    def merge(parts, axis):
        tp, tt, tw, sp, st = [lax.index_in_dim(parts, i, axis + 1, keepdims=False) for i in range(5)]
        tpm = jnp.max(tp, axis=axis, keepdims=True)
        spm = jnp.max(sp, axis=axis, keepdims=True)
        tr, sr = jnp.exp(tp - tpm), jnp.exp(sp - spm)
        return (
            jnp.squeeze(tpm, axis),
            jnp.sum(tt * tr, axis=axis),
            jnp.sum(tw * tr, axis=axis),
            jnp.squeeze(spm, axis),
            jnp.sum(st * sr, axis=axis),
        )

    everyone = lax.all_gather(stats, "vocab", axis=0).reshape(X, 2, 8, 2, J, hcnt)
    aligned = jnp.stack([everyone[:, 0], everyone[:, 1, :, ::-1]], axis=1)
    by_x = jnp.stack(merge(aligned, 1), axis=1).reshape(X, 5, 2, J, hcnt)
    neutral = jnp.array([-1e30, 0.0, 0.0, -1e30, 0.0], jnp.float32)[:, None, None]
    letters = []
    for b in range(En):
        xb, zb = set_of(b % Vn)
        letter = lax.dynamic_index_in_dim(by_x[xb], me ^ (b // Vn), 2, keepdims=False)
        letters.append(jnp.where(zl == zb, letter, neutral))
    mail = lax.all_to_all(jnp.stack(letters), "expert", split_axis=0, concat_axis=0, tiled=True)
    tp, tt, tw, sp, st = merge(mail, 0)
    kl = tw / tt - tp - jnp.log(tt) + sp + jnp.log(st)
    return kl.reshape(count)


def solution(mesh):
    in_specs = (
        P("expert", None),
        P("expert", None),
        P("expert", None),
        P("expert", None),
        P("expert", None, "vocab"),
        P("expert", "vocab", None),
        P(),
        P(),
        P(("vocab", "expert"), None),
        P(("vocab", "expert"), None),
    )
    out_specs = P("expert")

    return jax.shard_map(local, mesh=mesh, in_specs=in_specs, out_specs=out_specs, check_vma=False)
```

```python
import jax
import jax.numpy as jnp
from jax import lax
from jax.experimental import pallas as pl
from jax.experimental.pallas import tpu as pltpu
from jax.sharding import PartitionSpec as P


BOTH = ("expert", "vocab")

LIFT = 2.0**60
LIMIT = 8.0


def seats(expert, ranking, cap, kinds):
    numbers = jnp.arange(expert.shape[0], dtype=jnp.int32)
    same_expert = expert[:, None] == expert[None, :]
    before = ranking[None, :] < ranking[:, None]
    rank = jnp.sum(jnp.logical_and(same_expert, before).astype(jnp.int32), axis=1)
    kept = rank < cap
    earlier = jnp.logical_and(numbers[None, :] < numbers[:, None], jnp.logical_not(kept)[None, :])
    turn = jnp.sum(earlier.astype(jnp.int32), axis=1)
    kind = jnp.arange(kinds, dtype=jnp.int32)
    used = jnp.sum((expert[None, :] == kind[:, None]).astype(jnp.int32), axis=1)
    used = jnp.minimum(used, cap)
    start = jnp.sum(jnp.where(kind[None, :] < kind[:, None], cap - used[None, :], 0), axis=1)
    stop = start + cap - used
    fits = jnp.logical_and(turn[None, :] >= start[:, None], turn[None, :] < stop[:, None])
    spare = jnp.sum(jnp.where(fits, kind[:, None], 0), axis=0)
    slot = jnp.sum(jnp.where(fits, (used - start)[:, None] + turn[None, :], 0), axis=0)
    return jnp.where(kept, expert, spare), jnp.where(kept, rank, slot), kept


def ffn(rows, weight_in, weight_out):
    hidden = jax.nn.gelu(
        jnp.dot(rows, weight_in, preferred_element_type=jnp.float32)
    ).astype(jnp.bfloat16)
    return jnp.dot(hidden, weight_out, preferred_element_type=jnp.float32).astype(jnp.bfloat16)


def set_of(w):
    return (w & 1) | ((w >> 2) << 1), (w >> 1) & 1


def finish(where, gains, numbers, pools, t_shards, s_shards, count):
    width = gains.shape[-1]
    J = len(numbers)
    H = len(pools) // (2 * J)
    lanes = -(-count // 128) * 128
    rows = count * J
    tile = min(rows, 256)
    height = pools[0][0].shape[0]
    half = height // 2
    reach = height * len(pools)
    entries = t_shards[0].shape[0]
    span = entries * len(t_shards)
    shards = list(t_shards) + list(s_shards)
    counts = (J, len(pools), len(shards))

    def kernel(where_ref, gain_in, *refs):
        y, c, me, zh, zl = [where_ref[i] for i in range(5)]
        number_in, refs = refs[:J], refs[J:]
        pool_in, refs = refs[: 2 * counts[1]], refs[2 * counts[1] :]
        head_in, refs = refs[: counts[2]], refs[counts[2] :]
        out_ref, number, place, gain_ref, pool, head, normed, logits = refs[:8]
        small_sem, pool_sem, head_sem = refs[8:]
        copies = {}

        def begin(name, source, target, sem):
            copies[name] = pltpu.make_async_copy(source, target, sem)
            copies[name].start()

        def pool_copy(branch, i, kind):
            return pltpu.make_async_copy(
                pool_in[2 * i + kind],
                pool.at[branch, pl.ds(i * height, height)],
                pool_sem.at[branch, i],
            )

        def begin_pool(branch):
            for i in range(counts[1]):
                for kind in range(2):

                    @pl.when(y ^ branch == kind)
                    def _():
                        pool_copy(branch, i, kind).start()

        def begin_heads(branch):
            for i in range(counts[2] // 2):
                n = branch * (counts[2] // 2) + i
                begin(
                    ("head", n),
                    head_in[n],
                    head.at[branch, pl.ds(i * entries, entries)],
                    head_sem.at[n],
                )

        for i in range(J):
            begin(("number", i), number_in[i], number.at[i], small_sem.at[i])
        begin_pool(0)
        begin("gain", gain_in, gain_ref, small_sem.at[J])
        for i in range(J):
            copies["number", i].wait()
            values = number[i].astype(jnp.float32).astype(jnp.int32)
            table = []
            for branch in range(2):
                phase, side, round_, upper, low = [
                    values[5 * branch + n : 5 * branch + n + 1] for n in range(5)
                ]
                row = ((phase ^ me ^ i) * 2 + (side ^ c)) * H + (round_ ^ zh)
                row = row * height + (upper ^ zl) * half + low
                table.append(row.astype(jnp.float32))
            table.append(jnp.zeros((6, lanes), jnp.float32))
            column = jnp.concatenate(table, axis=0).T
            place[i * count : (i + 1) * count] = column[:count]
        for branch in range(2):
            for i in range(counts[1]):
                pool_copy(branch, i, 0).wait()
            if branch == 0:
                copies["gain"].wait()
                begin_pool(1)
            begin_heads(branch)
            for t in range(rows // tile):
                here = pl.ds(t * tile, tile)
                columns = lax.broadcasted_iota(jnp.int32, (tile, reach), 1).astype(jnp.float32)
                picked = jnp.where(columns == place[here, branch : branch + 1], 1.0, 0.0)
                total = jnp.dot(
                    picked.astype(jnp.bfloat16), pool[branch], preferred_element_type=jnp.float32
                )
                mean = jnp.mean(total * total, axis=-1, keepdims=True)
                scaled = total * lax.rsqrt(mean + 1e-05) * gain_ref[branch]
                normed[branch, here, :] = scaled.astype(jnp.bfloat16)
        for branch in range(2):
            for i in range(counts[2] // 2):
                copies["head", branch * (counts[2] // 2) + i].wait()
            for t in range(rows // 512):
                logits[branch, :, t*512:(t+1)*512] = lax.dot_general(
                    head[branch], normed[branch, t*512:(t+1)*512, :],
                    (((1,), (1,)), ((), ())),
                    preferred_element_type=jnp.float32,
                )
        for t in range(rows // 128):
            here = slice(t * 128, (t + 1) * 128)
            teacher, student = logits[0, :, here], logits[1, :, here]
            tp = jnp.max(teacher, axis=0, keepdims=True)
            sp = jnp.max(student, axis=0, keepdims=True)
            te = jnp.exp(teacher - tp)
            table = [
                tp,
                jnp.sum(te, axis=0, keepdims=True),
                jnp.sum(te * (teacher - student), axis=0, keepdims=True),
                sp,
                jnp.sum(jnp.exp(student - sp), axis=0, keepdims=True),
            ]
            out_ref[:, here] = jnp.concatenate(table + [jnp.zeros((3, 128), jnp.float32)], axis=0)

    return pl.pallas_call(
        kernel,
        in_specs=[
            pl.BlockSpec(memory_space=pltpu.SMEM),
        ]
        + [pl.BlockSpec(memory_space=pl.ANY)] * (sum(counts) + counts[1] + 1),
        out_specs=pl.BlockSpec(memory_space=pltpu.VMEM),
        out_shape=jax.ShapeDtypeStruct((8, rows), jnp.float32),
        scratch_shapes=[
            pltpu.VMEM((J, 16, lanes), jnp.bfloat16),
            pltpu.VMEM((rows, 8), jnp.float32),
            pltpu.VMEM(gains.shape, gains.dtype),
            pltpu.VMEM((2, reach, width), jnp.bfloat16),
            pltpu.VMEM((2, span, width), jnp.bfloat16),
            pltpu.VMEM((2, rows, width), jnp.bfloat16),
            pltpu.VMEM((2, span, rows), jnp.float32),
            pltpu.SemaphoreType.DMA((J + 1,)),
            pltpu.SemaphoreType.DMA((2, counts[1])),
            pltpu.SemaphoreType.DMA((counts[2],)),
        ],
        name="finish",
    )(where, gains, *numbers, *[a for pair in pools for a in pair], *shards)


def local(
    tokens,
    teacher_expert,
    student_expert,
    priority,
    expert_in,
    expert_out,
    teacher_gain,
    student_gain,
    teacher_head,
    student_head,
):
    count, width = tokens.shape
    En = lax.axis_size("expert")
    Vn = lax.axis_size("vocab")
    J = En // Vn
    H = En // 4
    X = Vn // 2
    cap = 3 * count // En
    hc = cap // 2
    e = lax.axis_index("expert")
    v = lax.axis_index("vocab")
    x, c = v // 2, v % 2
    zh, zl, y = e // 4, (e // 2) % 2, e % 2

    def by_expert(array, move):
        return lax.ppermute(array, "expert", [(s, move(s)) for s in range(En)])

    def by_vocab(array, move):
        perm = [(s, move(s)) for s in range(Vn)]
        return lax.ppermute(array, "vocab", [pair for pair in perm if pair[1] is not None])

    def by_both(array, move):
        perm = []
        for s in range(En):
            for u in range(Vn):
                target = move(s, u)
                if target is not None:
                    perm.append((s * Vn + u, target[0] * Vn + target[1]))
        return lax.ppermute(array, BOTH, perm)

    other_core = lambda array: by_vocab(array, lambda u: u ^ 1)

    ranking = priority[0]
    lifted = jnp.max(jnp.abs(tokens), axis=1).astype(jnp.float32) * LIFT
    lifted = jnp.where(lifted > LIMIT, LIFT, 0.0)
    group_rows = jnp.arange(En * hc, dtype=jnp.int32)[:, None]
    chosen = jnp.zeros((En * hc, count), jnp.float32)
    numbers = []
    for lane, expert in enumerate((teacher_expert[:, 0], student_expert[:, 0])):
        expert, slot, kept = seats(expert, ranking, cap, En // 2)
        source = 2 * expert + lane
        numbers += [source // Vn, source // 2 % 2, source // 4, slot // hc, slot % hc]
        place = jnp.where(slot // hc == c, (source ^ e) * hc + slot % hc, -1)
        weight = jnp.where(kept, 1.0, lifted)
        chosen = jnp.where(group_rows == place[None, :], weight[None, :], chosen)
    outgoing = jnp.dot(chosen.astype(jnp.bfloat16), tokens, preferred_element_type=jnp.float32)
    outgoing = outgoing.astype(jnp.bfloat16).reshape(En, hc, width)

    order = [m1 * 2 + (xi & 1) + ((xi >> 1) << 2) for m1 in range(2) for xi in range(X)]
    arrived = {0: outgoing[0]}
    for g in range(1, En):
        arrived[g] = by_expert(outgoing[g], lambda s: s ^ g)

    t_shards, s_shards = [teacher_head], [student_head]
    for d in range(1, X):
        t_shards.append(by_vocab(teacher_head, lambda u: u ^ (2 * d)))
        s_shards.append(by_vocab(student_head, lambda u: u ^ (2 * d)))
    s_far = by_expert(student_head, lambda s: s ^ 2)
    t_far = by_expert(teacher_head, lambda s: s ^ 2)
    t_diag = [by_expert(t_shards[d], lambda s: s ^ 2) for d in range(1, X)]
    s_diag = [by_vocab(s_far, lambda u: u ^ (2 * d)) for d in range(1, X)]
    t_shards += [t_far] + t_diag
    s_shards += [s_far] + s_diag

    def set_route(rho):
        def move(s, u):
            q = ((s // Vn) ^ rho) * Vn + u
            xd, zld = set_of(s % Vn)
            return (q >> 2) * 4 + zld * 2 + ((q >> 1) & 1), 2 * xd + (q & 1)

        return move

    numbers = jnp.stack(numbers).astype(jnp.bfloat16)
    numbers = jnp.pad(numbers, ((0, 16 - numbers.shape[0]), (0, -count % 128)))
    set_numbers = [by_both(numbers, set_route(rho)) for rho in range(J)]

    weight_in = expert_in[0]
    weight_out = expert_out[0]
    xe, _ = set_of(e % Vn)
    pools = []
    for r in range(J):
        own = jnp.stack([arrived[r * Vn + m] for m in order]).reshape(Vn * hc, width)
        rows = jnp.concatenate([own, other_core(own)], axis=0)
        partial = ffn(rows, weight_in, weight_out).reshape(2, 2, X, hc, width)
        kept_side = zl ^ c
        sent = lax.dynamic_index_in_dim(partial, 1 - kept_side, 1, keepdims=False)
        kept = lax.dynamic_index_in_dim(partial, kept_side, 1, keepdims=False)
        got = other_core(sent)
        summed = kept.astype(jnp.float32) + got[::-1].astype(jnp.float32)
        total = lax.dynamic_index_in_dim(summed, xe ^ x, 1, keepdims=False)
        narrow = summed.astype(jnp.bfloat16)
        for d in range(1, X):
            part = lax.dynamic_index_in_dim(narrow, xe ^ x ^ d, 1, keepdims=False)
            part = by_vocab(part, lambda u: u ^ (2 * d))
            total = total + part.astype(jnp.float32)
        own = lax.dynamic_index_in_dim(
            rows.reshape(2, 2, X, hc, width), kept_side, 1, keepdims=False
        )
        own = lax.dynamic_index_in_dim(own, xe ^ x, 1, keepdims=False).astype(jnp.float32)
        passing = jnp.max(jnp.abs(own), axis=-1, keepdims=True) > LIMIT
        total = jnp.where(passing, own * (1.0 / LIFT), own + total)
        reduced = total.astype(jnp.bfloat16).reshape(cap, width)
        mine, crossed = [], []
        for q in range(H):

            def spread(s, u):
                return ((s // 4) ^ q) * 4 + (u % 2) * 2 + s % 2, (u // 2) * 2 + (s // 2) % 2

            mine.append(by_both(reduced, spread))
            crossed.append(by_expert(mine[-1], lambda s: s ^ 1))
        pools += list(zip(mine, crossed))
        theirs = [other_core(mine[q]) for q in range(H)]
        far = [other_core(crossed[q]) for q in range(H)]
        pools += list(zip(theirs, far))

    me = ((zh * 2 + y) * 2 + c) // Vn
    stats = finish(
        jnp.stack([y, c, me, zh, zl]).astype(jnp.int32),
        jnp.stack([teacher_gain, student_gain])[:, None, :],
        set_numbers,
        pools,
        t_shards,
        s_shards,
        count,
    )

    def merge(parts, axis):
        tp, tt, tw, sp, st = [lax.index_in_dim(parts, i, axis + 1, keepdims=False) for i in range(5)]
        tpm = jnp.max(tp, axis=axis, keepdims=True)
        spm = jnp.max(sp, axis=axis, keepdims=True)
        tr, sr = jnp.exp(tp - tpm), jnp.exp(sp - spm)
        return (
            jnp.squeeze(tpm, axis),
            jnp.sum(tt * tr, axis=axis),
            jnp.sum(tw * tr, axis=axis),
            jnp.squeeze(spm, axis),
            jnp.sum(st * sr, axis=axis),
        )

    everyone = lax.all_gather(stats, "vocab", axis=0).reshape(X, 2, 8, J, count)
    by_x = jnp.stack(merge(everyone, 1), axis=1)
    neutral = jnp.array([-1e30, 0.0, 0.0, -1e30, 0.0], jnp.float32)[:, None]
    letters = []
    for b in range(En):
        xb, zb = set_of(b % Vn)
        letter = lax.dynamic_index_in_dim(by_x[xb], me ^ (b // Vn), 1, keepdims=False)
        letters.append(jnp.where(zl == zb, letter, neutral))
    mail = lax.all_to_all(jnp.stack(letters), "expert", split_axis=0, concat_axis=0, tiled=True)
    tp, tt, tw, sp, st = merge(mail, 0)
    return tw / tt - tp - jnp.log(tt) + sp + jnp.log(st)


def solution(mesh):
    in_specs = (
        P("expert", None),
        P("expert", None),
        P("expert", None),
        P("expert", None),
        P("expert", None, "vocab"),
        P("expert", "vocab", None),
        P(),
        P(),
        P(("vocab", "expert"), None),
        P(("vocab", "expert"), None),
    )
    out_specs = P("expert")

    return jax.shard_map(local, mesh=mesh, in_specs=in_specs, out_specs=out_specs, check_vma=False)
```

```python
import jax
import jax.numpy as jnp
from jax import lax
from jax.experimental import pallas as pl
from jax.experimental.pallas import tpu as pltpu
from jax.sharding import PartitionSpec as P


BOTH = ("expert", "vocab")

LIFT = 2.0**60
LIMIT = 8.0


def seats(expert, ranking, cap, kinds):
    numbers = jnp.arange(expert.shape[0], dtype=jnp.int32)
    same_expert = expert[:, None] == expert[None, :]
    before = ranking[None, :] < ranking[:, None]
    rank = jnp.sum(jnp.logical_and(same_expert, before).astype(jnp.int32), axis=1)
    kept = rank < cap
    earlier = jnp.logical_and(numbers[None, :] < numbers[:, None], jnp.logical_not(kept)[None, :])
    turn = jnp.sum(earlier.astype(jnp.int32), axis=1)
    kind = jnp.arange(kinds, dtype=jnp.int32)
    used = jnp.sum((expert[None, :] == kind[:, None]).astype(jnp.int32), axis=1)
    used = jnp.minimum(used, cap)
    start = jnp.sum(jnp.where(kind[None, :] < kind[:, None], cap - used[None, :], 0), axis=1)
    stop = start + cap - used
    fits = jnp.logical_and(turn[None, :] >= start[:, None], turn[None, :] < stop[:, None])
    spare = jnp.sum(jnp.where(fits, kind[:, None], 0), axis=0)
    slot = jnp.sum(jnp.where(fits, (used - start)[:, None] + turn[None, :], 0), axis=0)
    return jnp.where(kept, expert, spare), jnp.where(kept, rank, slot), kept


def ffn(rows, weight_in, weight_out):
    hidden = jax.nn.gelu(
        jnp.dot(rows, weight_in, preferred_element_type=jnp.float32)
    ).astype(jnp.bfloat16)
    return jnp.dot(hidden, weight_out, preferred_element_type=jnp.float32).astype(jnp.bfloat16)


def set_of(w):
    return (w & 1) | ((w >> 2) << 1), (w >> 1) & 1


def finish(where, gains, numbers, pools, t_shards, s_shards, count):
    width = gains.shape[-1]
    J = len(numbers)
    H = len(pools) // (2 * J)
    lanes = -(-count // 128) * 128
    rows = count * J
    tile = min(rows, 256)
    height = pools[0][0].shape[0]
    half = height // 2
    reach = height * len(pools)
    entries = t_shards[0].shape[0]
    span = entries * len(t_shards)
    shards = list(t_shards) + list(s_shards)
    counts = (J, len(pools), len(shards))

    def kernel(where_ref, gain_in, *refs):
        y, c, me, zh, zl = [where_ref[i] for i in range(5)]
        number_in, refs = refs[:J], refs[J:]
        pool_in, refs = refs[: 2 * counts[1]], refs[2 * counts[1] :]
        head_in, refs = refs[: counts[2]], refs[counts[2] :]
        out_ref, number, place, gain_ref, pool, head, normed, logits = refs[:8]
        small_sem, pool_sem, head_sem = refs[8:]
        copies = {}

        def begin(name, source, target, sem):
            copies[name] = pltpu.make_async_copy(source, target, sem)
            copies[name].start()

        def pool_copy(branch, i, kind):
            return pltpu.make_async_copy(
                pool_in[2 * i + kind],
                pool.at[branch, pl.ds(i * height, height)],
                pool_sem.at[branch, i],
            )

        def begin_pool(branch):
            for i in range(counts[1]):
                for kind in range(2):

                    @pl.when(y ^ branch == kind)
                    def _():
                        pool_copy(branch, i, kind).start()

        def begin_heads(branch):
            for i in range(counts[2] // 2):
                n = branch * (counts[2] // 2) + i
                begin(
                    ("head", n),
                    head_in[n],
                    head.at[branch, pl.ds(i * entries, entries)],
                    head_sem.at[n],
                )

        for i in range(J):
            begin(("number", i), number_in[i], number.at[i], small_sem.at[i])
        begin_pool(0)
        begin("gain", gain_in, gain_ref, small_sem.at[J])
        for i in range(J):
            copies["number", i].wait()
            values = number[i].astype(jnp.float32).astype(jnp.int32)
            table = []
            for branch in range(2):
                phase, side, round_, upper, low = [
                    values[5 * branch + n : 5 * branch + n + 1] for n in range(5)
                ]
                row = ((phase ^ me ^ i) * 2 + (side ^ c)) * H + (round_ ^ zh)
                row = row * height + (upper ^ zl) * half + low
                table.append(row.astype(jnp.float32))
            table.append(jnp.zeros((6, lanes), jnp.float32))
            column = jnp.concatenate(table, axis=0).T
            place[i * count : (i + 1) * count] = column[:count]
        for branch in range(2):
            for i in range(counts[1]):
                pool_copy(branch, i, 0).wait()
            if branch == 0:
                copies["gain"].wait()
                begin_pool(1)
            begin_heads(branch)
            for t in range(rows // tile):
                here = pl.ds(t * tile, tile)
                columns = lax.broadcasted_iota(jnp.int32, (tile, reach), 1).astype(jnp.float32)
                picked = jnp.where(columns == place[here, branch : branch + 1], 1.0, 0.0)
                total = jnp.dot(
                    picked.astype(jnp.bfloat16), pool[branch], preferred_element_type=jnp.float32
                )
                mean = jnp.mean(total * total, axis=-1, keepdims=True)
                scaled = total * lax.rsqrt(mean + 1e-05) * gain_ref[branch]
                normed[branch, here, :] = scaled.astype(jnp.bfloat16)
        for branch in range(2):
            for i in range(counts[2] // 2):
                copies["head", branch * (counts[2] // 2) + i].wait()
            logits[branch] = lax.dot_general(
                head[branch],
                normed[branch],
                (((1,), (1,)), ((), ())),
                preferred_element_type=jnp.float32,
            )
        for t in range(rows // 128):
            here = slice(t * 128, (t + 1) * 128)
            teacher, student = logits[0, :, here], logits[1, :, here]
            tp = jnp.max(teacher, axis=0, keepdims=True)
            sp = jnp.max(student, axis=0, keepdims=True)
            te = jnp.exp(teacher - tp)
            table = [
                tp,
                jnp.sum(te, axis=0, keepdims=True),
                jnp.sum(te * (teacher - student), axis=0, keepdims=True),
                sp,
                jnp.sum(jnp.exp(student - sp), axis=0, keepdims=True),
            ]
            out_ref[:, here] = jnp.concatenate(table + [jnp.zeros((3, 128), jnp.float32)], axis=0)

    return pl.pallas_call(
        kernel,
        in_specs=[
            pl.BlockSpec(memory_space=pltpu.SMEM),
        ]
        + [pl.BlockSpec(memory_space=pl.ANY)] * (sum(counts) + counts[1] + 1),
        out_specs=pl.BlockSpec(memory_space=pltpu.VMEM),
        out_shape=jax.ShapeDtypeStruct((8, rows), jnp.float32),
        scratch_shapes=[
            pltpu.VMEM((J, 16, lanes), jnp.bfloat16),
            pltpu.VMEM((rows, 8), jnp.float32),
            pltpu.VMEM(gains.shape, gains.dtype),
            pltpu.VMEM((2, reach, width), jnp.bfloat16),
            pltpu.VMEM((2, span, width), jnp.bfloat16),
            pltpu.VMEM((2, rows, width), jnp.bfloat16),
            pltpu.VMEM((2, span, rows), jnp.float32),
            pltpu.SemaphoreType.DMA((J + 1,)),
            pltpu.SemaphoreType.DMA((2, counts[1])),
            pltpu.SemaphoreType.DMA((counts[2],)),
        ],
        name="finish",
    )(where, gains, *numbers, *[a for pair in pools for a in pair], *shards)


def local(
    tokens,
    teacher_expert,
    student_expert,
    priority,
    expert_in,
    expert_out,
    teacher_gain,
    student_gain,
    teacher_head,
    student_head,
):
    count, width = tokens.shape
    En = lax.axis_size("expert")
    Vn = lax.axis_size("vocab")
    J = En // Vn
    H = En // 4
    X = Vn // 2
    cap = 3 * count // En
    hc = cap // 2
    e = lax.axis_index("expert")
    v = lax.axis_index("vocab")
    x, c = v // 2, v % 2
    zh, zl, y = e // 4, (e // 2) % 2, e % 2

    def by_expert(array, move):
        return lax.ppermute(array, "expert", [(s, move(s)) for s in range(En)])

    def by_vocab(array, move):
        perm = [(s, move(s)) for s in range(Vn)]
        return lax.ppermute(array, "vocab", [pair for pair in perm if pair[1] is not None])

    def by_both(array, move):
        perm = []
        for s in range(En):
            for u in range(Vn):
                target = move(s, u)
                if target is not None:
                    perm.append((s * Vn + u, target[0] * Vn + target[1]))
        return lax.ppermute(array, BOTH, perm)

    other_core = lambda array: by_vocab(array, lambda u: u ^ 1)

    ranking = priority[0]
    lifted = jnp.max(jnp.abs(tokens), axis=1).astype(jnp.float32) * LIFT
    lifted = jnp.where(lifted > LIMIT, LIFT, 0.0)
    group_rows = jnp.arange(En * hc, dtype=jnp.int32)[:, None]
    chosen = jnp.zeros((En * hc, count), jnp.float32)
    numbers = []
    for lane, expert in enumerate((teacher_expert[:, 0], student_expert[:, 0])):
        expert, slot, kept = seats(expert, ranking, cap, En // 2)
        source = 2 * expert + lane
        numbers += [source // Vn, source // 2 % 2, source // 4, slot // hc, slot % hc]
        place = jnp.where(slot // hc == c, (source ^ e) * hc + slot % hc, -1)
        weight = jnp.where(kept, 1.0, lifted)
        chosen = jnp.where(group_rows == place[None, :], weight[None, :], chosen)
    outgoing = jnp.dot(chosen.astype(jnp.bfloat16), tokens, preferred_element_type=jnp.float32)
    outgoing = outgoing.astype(jnp.bfloat16).reshape(En, hc, width)

    order = [m1 * 2 + (xi & 1) + ((xi >> 1) << 2) for m1 in range(2) for xi in range(X)]
    arrived = {0: outgoing[0]}
    for g in range(1, En):
        arrived[g] = by_expert(outgoing[g], lambda s: s ^ g)

    t_shards, s_shards = [teacher_head], [student_head]
    for d in range(1, X):
        t_shards.append(by_vocab(teacher_head, lambda u: u ^ (2 * d)))
        s_shards.append(by_vocab(student_head, lambda u: u ^ (2 * d)))
    s_far = by_expert(student_head, lambda s: s ^ 2)
    t_far = by_expert(teacher_head, lambda s: s ^ 2)
    t_diag = [by_expert(t_shards[d], lambda s: s ^ 2) for d in range(1, X)]
    s_diag = [by_vocab(s_far, lambda u: u ^ (2 * d)) for d in range(1, X)]
    t_shards += [t_far] + t_diag
    s_shards += [s_far] + s_diag

    def set_route(rho):
        def move(s, u):
            q = ((s // Vn) ^ rho) * Vn + u
            xd, zld = set_of(s % Vn)
            return (q >> 2) * 4 + zld * 2 + ((q >> 1) & 1), 2 * xd + (q & 1)

        return move

    numbers = jnp.stack(numbers).astype(jnp.bfloat16)
    numbers = jnp.pad(numbers, ((0, 16 - numbers.shape[0]), (0, -count % 128)))
    set_numbers = [by_both(numbers, set_route(rho)) for rho in range(J)]

    weight_in = expert_in[0]
    weight_out = expert_out[0]
    xe, _ = set_of(e % Vn)
    pools = []
    for r in range(J):
        own = jnp.stack([arrived[r * Vn + m] for m in order]).reshape(Vn * hc, width)
        rows = jnp.concatenate([own, other_core(own)], axis=0)
        partial = ffn(rows, weight_in, weight_out).reshape(2, 2, X, hc, width)
        kept_side = zl ^ c
        sent = lax.dynamic_index_in_dim(partial, 1 - kept_side, 1, keepdims=False)
        kept = lax.dynamic_index_in_dim(partial, kept_side, 1, keepdims=False)
        got = other_core(sent)
        summed = kept.astype(jnp.float32) + got[::-1].astype(jnp.float32)
        total = lax.dynamic_index_in_dim(summed, xe ^ x, 1, keepdims=False)
        narrow = summed.astype(jnp.bfloat16)
        for d in range(1, X):
            part = lax.dynamic_index_in_dim(narrow, xe ^ x ^ d, 1, keepdims=False)
            part = by_vocab(part, lambda u: u ^ (2 * d))
            total = total + part.astype(jnp.float32)
        own = lax.dynamic_index_in_dim(
            rows.reshape(2, 2, X, hc, width), kept_side, 1, keepdims=False
        )
        own = lax.dynamic_index_in_dim(own, xe ^ x, 1, keepdims=False).astype(jnp.float32)
        passing = jnp.max(jnp.abs(own), axis=-1, keepdims=True) > LIMIT
        total = jnp.where(passing, own * (1.0 / LIFT), own + total)
        reduced = total.astype(jnp.bfloat16).reshape(cap, width)
        mine, crossed = [], []
        for q in range(H):

            def spread(s, u):
                return ((s // 4) ^ q) * 4 + (u % 2) * 2 + s % 2, (u // 2) * 2 + (s // 2) % 2

            mine.append(by_both(reduced, spread))
            crossed.append(by_expert(mine[-1], lambda s: s ^ 1))
        pools += list(zip(mine, crossed))
        theirs = [other_core(mine[q]) for q in range(H)]
        far = [other_core(crossed[q]) for q in range(H)]
        pools += list(zip(theirs, far))

    me = ((zh * 2 + y) * 2 + c) // Vn
    stats = finish(
        jnp.stack([y, c, me, zh, zl]).astype(jnp.int32),
        jnp.stack([teacher_gain, student_gain])[:, None, :],
        set_numbers,
        pools,
        t_shards,
        s_shards,
        count,
    )

    def merge(parts, axis):
        tp, tt, tw, sp, st = [lax.index_in_dim(parts, i, axis + 1, keepdims=False) for i in range(5)]
        tpm = jnp.max(tp, axis=axis, keepdims=True)
        spm = jnp.max(sp, axis=axis, keepdims=True)
        tr, sr = jnp.exp(tp - tpm), jnp.exp(sp - spm)
        return (
            jnp.squeeze(tpm, axis),
            jnp.sum(tt * tr, axis=axis),
            jnp.sum(tw * tr, axis=axis),
            jnp.squeeze(spm, axis),
            jnp.sum(st * sr, axis=axis),
        )

    everyone = lax.all_gather(stats, "vocab", axis=0).reshape(X, 2, 8, J, count)
    by_x = jnp.stack(merge(everyone, 1), axis=1)
    neutral = jnp.array([-1e30, 0.0, 0.0, -1e30, 0.0], jnp.float32)[:, None]
    letters = []
    for b in range(En):
        xb, zb = set_of(b % Vn)
        letter = lax.dynamic_index_in_dim(by_x[xb], me ^ (b // Vn), 1, keepdims=False)
        letters.append(jnp.where(zl == zb, letter, neutral))
    mail = lax.all_to_all(jnp.stack(letters), "expert", split_axis=0, concat_axis=0, tiled=True)
    tp, tt, tw, sp, st = merge(mail, 0)
    return tw / tt - tp - jnp.log(tt) + sp + jnp.log(st)


def solution(mesh):
    in_specs = (
        P("expert", None),
        P("expert", None),
        P("expert", None),
        P("expert", None),
        P("expert", None, "vocab"),
        P("expert", "vocab", None),
        P(),
        P(),
        P(("vocab", "expert"), None),
        P(("vocab", "expert"), None),
    )
    out_specs = P("expert")

    return jax.shard_map(local, mesh=mesh, in_specs=in_specs, out_specs=out_specs, check_vma=False)
```
